256 devices in a mesh: rows: 64 (over z, x, core), cols: 4 (over y).
Axes of the slice: x: 4, y: 4, z: 8, core: 2. Of those that a mesh axis runs over, the one named last changes fastest.
Arguments:
- source: float32 [8192, 32768], P('rows', 'cols'), may hold values from -6 to 6
- low_row: int32 [8192], replicated, may hold values from 0 to 8190, as said below
- weight_low: float32 [8192], replicated, may hold values from 0 to 1
Outputs:
- mercator: float32 [8192, 32768], P('rows', 'cols')
- level1: float32 [4096, 16384], P('rows', 'cols')
- level2: float32 [2048, 8192], P('rows', 'cols')
- level3: float32 [1024, 4096], P(('rows', 'cols'))
- level4: float32 [512, 2048], P(('rows', 'cols'))
The draws below stay inside these ranges and needn't reach their ends.
Inputs may be any that keep to these rules, and one draw needn't show every extreme that they name: With t = 68 degrees in radians, E = ln tan(pi/4 + t/2), y = E * (1 - (2m + 1) / 16384) and lat = 2 atan(exp(y)) - pi/2, the base row of Mercator row m is floor((t - lat) / t * 8192 - 0.5) clipped to the range; low_row[m] differs from it by at most 2 and is then clipped to the range.
All inputs are finite; a program needn't handle non-finite values.
Results may differ from the reference program's by a relative error of at most 0.00007.
Values sent between devices are 32-bit elements; how exact they have to be, the bound alone decides.
No kernel may reach another device: no remote copies, remote signals or barrier semaphores. Data moves between devices by JAX's collectives and lax.ppermute only.
A program may use at most 128 MiB of HBM per device.

```python
import math
import jax
import jax.numpy as jnp

TOTAL = 8192
COLS = 32768


def draw_low_row(key, part):
    window_top = 68.0 * math.pi / 180.0
    north_edge = math.log(math.tan(math.pi / 4 + window_top / 2))
    centres = (2.0 * jnp.arange(TOTAL, dtype=jnp.float32) + 1.0) / (2.0 * TOTAL)
    merc_y = north_edge * (1.0 - centres)
    latitude = 2.0 * jnp.arctan(jnp.exp(merc_y)) - math.pi / 2
    position = (window_top - latitude) / window_top * TOTAL - 0.5
    base_rows = jnp.clip(jnp.floor(position), 0, TOTAL - 2).astype(jnp.int32)
    jitter = jax.random.randint(key, (TOTAL,), -2, 3, dtype=jnp.int32)
    return jnp.clip(base_rows + jitter, 0, TOTAL - 2).astype(jnp.int32)


def shard_levels(rng, extent, shards, low, high):
    def one(axis_at, shards_of):
        draws = jax.random.uniform(jax.random.fold_in(jax.random.fold_in(rng, 6), axis_at), (shards_of,), jnp.float32, low / len(shards), high / len(shards))
        return jnp.repeat(jnp.exp(draws), extent[axis_at] // shards_of).reshape((-1,) + (1,) * (len(extent) - axis_at - 1))

    loudness = one(*shards[0])
    for cut in shards[1:]:
        loudness = loudness * one(*cut)
    return loudness


def normal_values(key, dims, width, reach, split=(), kind=jnp.bfloat16):
    entries = width * jax.random.normal(key, dims, jnp.float32)
    if split:
        entries = entries * shard_levels(key, dims, split, -0.22, 0.18)
    return jnp.clip(entries, -reach, reach).astype(kind)


def setup_inputs(seed: int = 0) -> dict:
    arg_keys = jax.random.split(jax.random.key(seed), 4)
    return {
        "source": normal_values(arg_keys[0], (TOTAL, COLS), 1.0, 6.0, ((0, 64), (1, 4)), jnp.float32),
        "low_row": draw_low_row(jax.random.fold_in(arg_keys[3], 71), 0),
        "weight_low": jnp.clip(jax.random.uniform(arg_keys[2], (TOTAL,), jnp.float32, 0.0, 1.0), 0.0, 1.0),
    }


def blend(columns, low_row, weight_low):
    upper_rows = jnp.take(columns, low_row, axis=0)
    lower_rows = jnp.take(columns, low_row + 1, axis=0)
    scales = weight_low.reshape((-1,) + (1,) * (columns.ndim - 1))
    return scales * upper_rows + (1.0 - scales) * lower_rows


def halve(picture):
    return (picture[0::2, 0::2] + picture[1::2, 0::2] + picture[0::2, 1::2] + picture[1::2, 1::2]) * 0.25


def reference(source, low_row, weight_low):
    mercator = blend(source, low_row, weight_low)
    level1 = halve(mercator)
    level2 = halve(level1)
    level3 = halve(level2)
    level4 = halve(level3)
    return (mercator, level1, level2, level3, level4)
```

```python
import math

import jax
import jax.numpy as jnp
import numpy as np
from jax import lax
from jax.experimental import pallas as pl
from jax.experimental.pallas import tpu as pltpu
from jax.sharding import PartitionSpec as P


TOTAL = 8192
ROWS = 64
OWN = TOTAL // ROWS
CODE = 1024

STOPS = {
    'D': (),
    'P': ((0, 1),),
    'M': ((0, -1),),
}
CLASSES = (('D', 16, 7), ('D', 8, 6), ('P', 16, 2), ('M', 16, 2))
ROUTES = (
    3, 35, 516, 33281, 33797, 34305, 34341, 67073, 67105, 67589, 68097, 68131,
    100866, 100898, 101381, 101409, 101922, 134659, 134692, 135172, 167938, 168451, 168485, 168962,
    201732, 201761, 202243, 202275, 235009, 235041, 235526, 236065, 236097, 268805, 269314, 269348,
    302082, 302113, 302597, 302626, 303137, 335393, 335877, 335905, 335969, 336386, 336417, 369155,
    369187, 369668, 402433, 402468, 402950, 435745, 435777, 436230, 436289, 436737, 469510, 469537,
    470017, 470081, 502789, 502817, 503297, 503329, 503362, 536067, 536099, 536580, 536609, 569347,
    569377, 569860, 569891, 602625, 602659, 603141, 603170, 635940, 636422, 636449, 669185, 669217,
    669702, 669730, 702465, 702982, 703011, 735809, 736263, 736290, 769058, 769542, 769572, 802305,
    802822, 802851, 835585, 836102, 836130, 868865, 868897, 869382, 869410, 902145, 902178, 902662,
    935425, 935459, 935941, 935969, 968706, 968738, 969221, 1001986, 1002020, 1002499, 1002530, 1035268,
    1035298, 1035778, 1035810, 1068549, 1068578, 1069058, 1101829, 1101860, 1102337, 1135109, 1135141, 1167873,
    1168389, 1168419, 1201154, 1201185, 1201669, 1234434, 1234468, 1234947, 1234977, 1267716, 1267747, 1268226,
    1300997, 1301028, 1301537, 1333793, 1334279, 1367076, 1367557, 1400322, 1400355, 1400834, 1400865, 1400929,
    1433604, 1433633, 1433697, 1434145, 1434209, 1466887, 1499713, 1500166, 1532929, 1532963, 1533443, 1533474,
    1566212, 1566241, 1566721, 1566755, 1599494, 1599521, 1632289, 1632774, 1632801, 1665537, 1665571, 1666052,
    1666081, 1698819, 1698851, 1699329, 1699363, 1732102, 1732129, 1764897, 1765382, 1798145, 1798179, 1798660,
    1831427, 1831460, 1831938, 1864708, 1864741, 1897473, 1897988, 1898019, 1930755, 1930785, 1931267, 1931297,
    1964036, 1964067, 1964545, 1997316, 1997349, 2030082, 2030595, 2030628, 2063364, 2063873, 2063907, 2096646,
)


def row_bounds():
    top = 68.0 * math.pi / 180.0
    edge = math.log(math.tan(math.pi / 4 + top / 2))
    y = edge * (1 - (2 * np.arange(TOTAL) + 1) / (2.0 * TOTAL))
    position = (top - (2 * np.arctan(np.exp(y)) - math.pi / 2)) / top * TOTAL - 0.5
    low = np.clip(np.floor(position - 0.05), 0, TOTAL - 2) - 2
    high = np.clip(np.floor(position + 0.05), 0, TOTAL - 2) + 2
    return np.clip(low, 0, TOTAL - 2).astype(int), np.clip(high, 0, TOTAL - 2).astype(int)


def wanted(low, high):
    out = {}
    for d in range(ROWS):
        mine = range(OWN * d, OWN * d + OWN)
        first, last = low[mine[0]], high[mine[-1]] + 1
        for s in range(first // OWN, last // OWN + 1):
            begin, end = s * OWN, s * OWN + OWN - 1
            plain = [("s", r) for r in range(max(first, begin), min(last, end) + 1)]
            inside = [m for m in mine if low[m] >= begin and high[m] + 1 <= end]
            across = sorted({
                r for m in mine if m not in inside for r in range(low[m], high[m] + 2) if r // OWN == s
            })
            mixed = [("s", r) for r in across if r < begin + OWN // 2]
            mixed += [("m", m) for m in inside]
            mixed += [("s", r) for r in across if r >= begin + OWN // 2]
            out[s, d] = plain if len(plain) <= len(mixed) else mixed
    return out


def stop(q, dz, dx):
    z, x = q // 8, q % 8 // 2
    return (z + dz) % 8 * 8 + (x + dx) % 4 * 2 + q % 2


def colour(edges, count):
    at_s, at_d = {}, {}
    for s, d in edges:
        a = next(c for c in range(count) if (s, c) not in at_s)
        b = next(c for c in range(count) if (d, c) not in at_d)
        if a != b:
            path, node, side, c = [], d, 1, a
            while True:
                table = at_d if side else at_s
                if (node, c) not in table:
                    break
                other = table[node, c]
                path.append((other, node, c) if side else (node, other, c))
                node, side, c = other, 1 - side, a + b - c
            for u, v, k in path:
                del at_s[u, k], at_d[v, k]
            for u, v, k in path:
                at_s[u, a + b - k], at_d[v, a + b - k] = v, u
        at_s[s, a], at_d[d, a] = d, s
    return [sorted((s, d) for (s, k), d in at_s.items() if k == c) for c in range(count)]


def make_plan():
    low, high = row_bounds()
    items = wanted(low, high)
    by_class = [[] for _ in CLASSES]
    for code in ROUTES:
        blocks, kind, d, s = code % 32, code // 32 % 16, code // 512 % 64, code // 32768
        by_class[kind] += [(s, d)] * blocks
    slots, left = [], {e: list(v) for e, v in items.items()}
    for (kind, size, count), edges in zip(CLASSES, by_class):
        for pairs in colour(edges, count):
            if pairs:
                slots.append((kind, size, pairs))
    slots.sort(key=lambda t: (-len(STOPS[t[0]]), -t[1]))
    total = sum(size for _, size, _ in slots)
    send = np.zeros((ROWS, 1, total), np.int32)
    merc = np.full((ROWS, OWN), -1, np.int32)
    base = np.array([low[OWN * d] for d in range(ROWS)])
    width = max(high[OWN * d + OWN - 1] + 2 - base[d] for d in range(ROWS))
    place = np.zeros((ROWS, width), np.int32)
    used = np.zeros((ROWS, len(slots)), np.int32)
    at = 0
    for j, (kind, size, pairs) in enumerate(slots):
        for s, d in pairs:
            block, left[s, d] = left[s, d][:size], left[s, d][size:]
            used[d, j] = 1 if block else 0
            for k, (what, r) in enumerate(block):
                if what == "m":
                    send[s, 0, at + k] = CODE + r
                    merc[d, r - OWN * d] = at + k
                else:
                    send[s, 0, at + k] = r - OWN * s
                    place[d, r - base[d]] = at + k
        at += size
    assert not any(left.values())
    take = np.concatenate([used, base[:, None].astype(np.int32), merc, place], axis=1)[:, None, :]
    return slots, send, take.astype(np.int32)


def hops(slot):
    kind, _, pairs = slot
    tracks = []
    for s, d in pairs:
        track = [s]
        for dz, dx in STOPS[kind]:
            track.append(stop(track[-1], dz, dx))
        tracks.append(track + [d])
    return [[(t[i], t[i + 1]) for t in tracks] for i in range(len(STOPS[kind]) + 1)]


def pack_rows(slots, first, source, send, me, low_row, weight_low):
    sizes = [size for _, size, _ in slots]

    def kernel(me_ref, send_ref, low_ref, weight_ref, source_ref, *outs):
        begin = me_ref[0] * OWN
        at = first
        for out, size in zip(outs, sizes):

            def row(k, _, out=out, at=at):
                code = send_ref[0, 0, at + k]
                mixed = code >= CODE
                m = jnp.maximum(code - CODE, 0)
                r0 = jnp.where(mixed, low_ref[m] - begin, code)
                r0 = jnp.clip(r0, 0, OWN - 1)
                r1 = jnp.where(mixed, jnp.minimum(r0 + 1, OWN - 1), r0)
                w = jnp.where(mixed, weight_ref[m], 1.0)
                v = 1.0 - w
                b0 = lax.div(r0, 8) * 512 + lax.rem(r0, 8)
                b1 = lax.div(r1, 8) * 512 + lax.rem(r1, 8)
                for j in range(8):
                    a = source_ref[pl.ds(b0 + 64 * j, 8, stride=8), :]
                    b = source_ref[pl.ds(b1 + 64 * j, 8, stride=8), :]
                    out[pl.ds(pl.multiple_of(k * 64 + 8 * j, 8), 8), :] = w * a + v * b
                return 0

            lax.fori_loop(0, size, row, 0, unroll=4)
            at += size

    total = send.shape[-1]
    return pl.pallas_call(
        kernel,
        grid_spec=pltpu.PrefetchScalarGridSpec(
            num_scalar_prefetch=1,
            grid=(1,),
            in_specs=[
                pl.BlockSpec((1, 1, total), lambda i, q: (q[0], 0, 0), memory_space=pltpu.SMEM),
                pl.BlockSpec(memory_space=pltpu.SMEM),
                pl.BlockSpec(memory_space=pltpu.SMEM),
                pl.BlockSpec((TOTAL, 128), lambda i, q: (0, 0)),
            ],
            out_specs=[pl.BlockSpec((size * 64, 128), lambda i, q: (0, 0)) for size in sizes],
        ),
        out_shape=[jax.ShapeDtypeStruct((size * 64, 128), jnp.float32) for size in sizes],
        compiler_params=pltpu.CompilerParams(vmem_limit_bytes=40 << 20),
        name="pack_rows",
    )(me, send, low_row, weight_low, source)


def finish(slots, blocks, take, me, low_row, weight_low):
    sizes = [size for _, size, _ in slots]
    starts = np.cumsum([0] + sizes)
    n = len(slots)
    width = take.shape[-1] - n - 1 - OWN

    def pooled(sums, rows):
        pair = jnp.concatenate([sums[pl.ds(0, rows // 2, stride=2), :], sums[pl.ds(1, rows // 2, stride=2), :]], axis=1)
        lane = lax.broadcasted_iota(jnp.int32, (256, 128), 0)
        to = lax.broadcasted_iota(jnp.int32, (256, 128), 1)
        pairing = jnp.where(lax.div(lane, 2) == to, 0.25, 0.0).astype(jnp.bfloat16)
        high = pair.astype(jnp.bfloat16)
        rest = pair - high.astype(jnp.float32)
        middle = rest.astype(jnp.bfloat16)
        low = (rest - middle.astype(jnp.float32)).astype(jnp.bfloat16)
        return sum(jnp.dot(part, pairing, preferred_element_type=jnp.float32) for part in (low, middle, high))

    def kernel(me_ref, take_ref, low_ref, weight_ref, *refs):
        ins, (out, out1, out2, small, got, sums, sems) = refs[:n], refs[n:]
        step = pl.program_id(0)

        @pl.when(step == 0)
        def _():
            def copy(j):
                return pltpu.make_async_copy(ins[j], got.at[pl.ds(int(starts[j]) * 64, sizes[j] * 64), :], sems.at[j])

            for j in range(n):
                copy(j).start()
            for j in range(n):
                copy(j).wait()

        base = take_ref[0, 0, n]

        def blended(r):
            i = step * 32 + r
            fixed = take_ref[0, 0, n + 1 + i]
            m = me_ref[0] * OWN + i
            c = jnp.clip(low_ref[m] - base, 0, width - 2)
            p0 = take_ref[0, 0, n + 1 + OWN + c]
            p1 = take_ref[0, 0, n + 2 + OWN + c]
            done = fixed >= 0
            p0 = jnp.where(done, fixed, p0)
            p1 = jnp.where(done, fixed, p1)
            w = jnp.where(done, 1.0, weight_ref[m])
            v = 1.0 - w
            for j in range(8):
                a = got[pl.ds(pl.multiple_of(p0 * 64 + 8 * j, 8), 8), :]
                b = got[pl.ds(pl.multiple_of(p1 * 64 + 8 * j, 8), 8), :]
                yield j, w * a + v * b

        for r in range(0, 32, 2):
            for (j, a), (_, b) in zip(blended(r), blended(r + 1)):
                out[pl.ds(r // 8 * 512 + r % 8 + 64 * j, 8, stride=8), :] = a
                out[pl.ds(r // 8 * 512 + r % 8 + 1 + 64 * j, 8, stride=8), :] = b
                sums[pl.ds(r * 32 + 8 * j, 8), :] = a + b
        one = pooled(sums, 1024)
        for r in range(16):
            for j in range(4):
                out1[pl.ds(r // 8 * 256 + r % 8 + 64 * j, 8, stride=8), :] = one[r * 32 + 8 * j : r * 32 + 8 * j + 8]
        for r in range(8):
            sums[pl.ds(r * 32, 32), :] = one[r * 64 : r * 64 + 32] + one[r * 64 + 32 : r * 64 + 64]
        two = pooled(sums, 256)
        for r in range(8):
            for j in range(2):
                out2[pl.ds(r + 64 * j, 8, stride=8), :] = two[r * 16 + 8 * j : r * 16 + 8 * j + 8]
        for r in range(4):
            sums[pl.ds(r * 16, 16), :] = two[r * 32 : r * 32 + 16] + two[r * 32 + 16 : r * 32 + 32]
        three = pooled(sums, 64)
        small[0, pl.ds(0, 32), :] = three
        for r in range(2):
            sums[pl.ds(r * 8, 8), :] = three[r * 16 : r * 16 + 8] + three[r * 16 + 8 : r * 16 + 16]
        small[0, pl.ds(32, 8), :] = pooled(sums, 16)

    return pl.pallas_call(
        kernel,
        grid_spec=pltpu.PrefetchScalarGridSpec(
            num_scalar_prefetch=1,
            grid=(4,),
            in_specs=[
                pl.BlockSpec((1, 1, take.shape[-1]), lambda i, q: (q[0], 0, 0), memory_space=pltpu.SMEM),
                pl.BlockSpec(memory_space=pltpu.SMEM),
                pl.BlockSpec(memory_space=pltpu.SMEM),
            ]
            + [pl.BlockSpec(memory_space=pl.ANY)] * n,
            out_specs=[
                pl.BlockSpec((2048, 128), lambda i, q: (i, 0)),
                pl.BlockSpec((512, 128), lambda i, q: (i, 0)),
                pl.BlockSpec((128, 128), lambda i, q: (i, 0)),
                pl.BlockSpec((1, 40, 128), lambda i, q: (i, 0, 0)),
            ],
            scratch_shapes=[
                pltpu.VMEM((int(starts[-1]) * 64, 128), jnp.float32),
                pltpu.VMEM((1024, 128), jnp.float32),
                pltpu.SemaphoreType.DMA((n,)),
            ],
        ),
        out_shape=[
            jax.ShapeDtypeStruct((8192, 128), jnp.float32),
            jax.ShapeDtypeStruct((2048, 128), jnp.float32),
            jax.ShapeDtypeStruct((512, 128), jnp.float32),
            jax.ShapeDtypeStruct((4, 40, 128), jnp.float32),
        ],
        compiler_params=pltpu.CompilerParams(
            dimension_semantics=("arbitrary",), vmem_limit_bytes=40 << 20
        ),
        name="finish",
    )(me, take, low_row, weight_low, *blocks)


def tiled(flat, rows, cols):
    return flat.reshape(rows // 8, cols // 128, 8, 128).transpose(0, 2, 1, 3).reshape(rows, cols)


def solution(mesh):
    slots, send, take = make_plan()
    groups = [slots]

    def body(source, low_row, weight_low):
        me = lax.axis_index("rows").astype(jnp.int32).reshape(1)
        flat = source.reshape(16, 8, 64, 128).transpose(0, 2, 1, 3).reshape(TOTAL, 128)
        packed = []
        at = 0
        for group in groups:
            packed += pack_rows(group, at, flat, send, me, low_row, weight_low)
            at += sum(size for _, size, _ in group)
        blocks = [[b] for b in packed]
        tracks = [hops(slot) for slot in slots]
        for i in range(max(len(t) for t in tracks)):
            for block, track in zip(blocks, tracks):
                if i < len(track):
                    block.append(lax.ppermute(block[-1], "rows", track[i]))
        out, out1, out2, small = finish(slots, [b[-1] for b in blocks], take, me, low_row, weight_low)
        pieces = lax.all_to_all(small, "cols", split_axis=0, concat_axis=0, tiled=True)
        level3 = pieces[:, :32].reshape(4, 4, 1024).transpose(1, 0, 2).reshape(4, 4096)
        level4 = pieces[:, 32:].reshape(4, 2, 512).transpose(1, 0, 2).reshape(2, 2048)
        return (
            tiled(out, 128, 8192),
            tiled(out1, 64, 4096),
            tiled(out2, 32, 2048),
            level3,
            level4,
        )

    return jax.shard_map(
        body,
        mesh=mesh,
        in_specs=(P("rows", "cols"), P(), P()),
        out_specs=(
            P("rows", "cols"),
            P("rows", "cols"),
            P("rows", "cols"),
            P(("rows", "cols"), None),
            P(("rows", "cols"), None),
        ),
        check_vma=False,
    )
```

```python
import math

import jax
import jax.numpy as jnp
import numpy as np
from jax import lax
from jax.experimental import pallas as pl
from jax.experimental.pallas import tpu as pltpu
from jax.sharding import PartitionSpec as P


TOTAL = 8192
ROWS = 64
OWN = TOTAL // ROWS
SLOTS = (9, 10, 11, 12, 0, 1, 2, 3, 4, 5, 6, 7, 8)
ISSUE = (0, 2, 4, 6, 8, 10, 12, 14, 16, 18, 20, 22, 24, 1, 3, 5, 7)
SPAN = 3
CODE = 1024

STOPS = {
    "D": (),
    "P": ((0, 1),),
    "M": ((0, -1),),
    "V": ((1, -1),),
    "Y": ((-1, -1),),
}
CLASSES = (("D", 32, 3), ("D", 16, 3), ("D", 8, 3), ("P", 32, 1), ("M", 32, 1), ("Y", 16, 1), ("V", 16, 1))
ROUTES = (
    2, 65, 513, 545, 578, 33313, 33794, 33825, 34305, 34337, 34369, 67105,
    67137, 67586, 67617, 68097, 68161, 100865, 100930, 101378, 101409, 101441, 101921, 134657,
    134690, 134722, 135170, 167937, 168449, 168482, 168515, 168961, 201762, 201793, 201825, 202242,
    202305, 235073, 235169, 235522, 235554, 236065, 236097, 268802, 268833, 269313, 269345, 269378,
    302114, 302145, 302595, 303169, 335425, 335874, 335937, 336001, 336385, 336449, 369186, 369217,
    369281, 369666, 402467, 402947, 435779, 436226, 436353, 436385, 436769, 469507, 469569, 470049,
    470082, 502786, 502817, 502849, 503329, 503361, 503393, 536065, 536098, 536129, 536578, 536641,
    569345, 569377, 569409, 569858, 569889, 569921, 602658, 602689, 603139, 635937, 635970, 636418,
    636450, 636481, 669217, 669249, 669698, 669730, 669762, 702497, 702979, 703043, 735777, 736258,
    736290, 736353, 769090, 769539, 769570, 802370, 802819, 802849, 802881, 835617, 836098, 836130,
    836162, 868897, 868929, 869378, 869410, 869442, 902145, 902657, 902691, 902722, 935425, 935489,
    935938, 935969, 936001, 968705, 968737, 969217, 969250, 969282, 1001986, 1002497, 1002529, 1002562,
    1035266, 1035297, 1035777, 1035842, 1068546, 1068578, 1069057, 1101826, 1101859, 1102402, 1135107, 1135137,
    1135169, 1167905, 1168386, 1168418, 1168449, 1201153, 1201217, 1201665, 1201699, 1234434, 1234945, 1234977,
    1235009, 1267714, 1267745, 1267777, 1268258, 1300995, 1301025, 1301569, 1333825, 1334275, 1334338, 1367074,
    1367554, 1367713, 1400353, 1400385, 1400417, 1400897, 1400961, 1400993, 1433601, 1433635, 1433665, 1434177,
    1434273, 1466883, 1466913, 1499681, 1500163, 1532962, 1532993, 1533442, 1566209, 1566273, 1566305, 1566721,
    1566785, 1599490, 1599521, 1599553, 1599681, 1632321, 1632771, 1632833, 1665570, 1665601, 1666049, 1666113,
    1666209, 1666241, 1698818, 1698881, 1699361, 1699393, 1699521, 1732098, 1732130, 1732161, 1764929, 1765378,
    1765409, 1765537, 1798178, 1798209, 1798657, 1798753, 1831426, 1831457, 1831969, 1832002, 1864707, 1864769,
    1897505, 1897986, 1898017, 1898049, 1930753, 1930785, 1930817, 1931265, 1931297, 1931329, 1964034, 1964065,
    1964097, 1964610, 1997314, 1997346, 1997377, 2030081, 2030593, 2030626, 2030658, 2063362, 2063873, 2063937,
    2096642, 2096674,
)


def row_bounds():
    top = 68.0 * math.pi / 180.0
    edge = math.log(math.tan(math.pi / 4 + top / 2))
    y = edge * (1 - (2 * np.arange(TOTAL) + 1) / (2.0 * TOTAL))
    position = (top - (2 * np.arctan(np.exp(y)) - math.pi / 2)) / top * TOTAL - 0.5
    low = np.clip(np.floor(position - 0.05), 0, TOTAL - 2) - 2
    high = np.clip(np.floor(position + 0.05), 0, TOTAL - 2) + 2
    return np.clip(low, 0, TOTAL - 2).astype(int), np.clip(high, 0, TOTAL - 2).astype(int)


def wanted(low, high):
    out = {}
    for d in range(ROWS):
        mine = range(OWN * d, OWN * d + OWN)
        first, last = low[mine[0]], high[mine[-1]] + 1
        for s in range(first // OWN, last // OWN + 1):
            begin, end = s * OWN, s * OWN + OWN - 1
            plain = [("s", r) for r in range(max(first, begin), min(last, end) + 1)]
            inside = [m for m in mine if low[m] >= begin and high[m] + 1 <= end]
            across = sorted({
                r for m in mine if m not in inside for r in range(low[m], high[m] + 2) if r // OWN == s
            })
            mixed = [("s", r) for r in across if r < begin + OWN // 2]
            mixed += [("m", m) for m in inside]
            mixed += [("s", r) for r in across if r >= begin + OWN // 2]
            out[s, d] = plain if len(plain) <= len(mixed) else mixed
    return out


def stop(q, dz, dx):
    z, x = q // 8, q % 8 // 2
    return (z + dz) % 8 * 8 + (x + dx) % 4 * 2 + q % 2


def colour(edges, count):
    at_s, at_d = {}, {}
    for s, d in edges:
        a = next(c for c in range(count) if (s, c) not in at_s)
        b = next(c for c in range(count) if (d, c) not in at_d)
        if a != b:
            path, node, side, c = [], d, 1, a
            while True:
                table = at_d if side else at_s
                if (node, c) not in table:
                    break
                other = table[node, c]
                path.append((other, node, c) if side else (node, other, c))
                node, side, c = other, 1 - side, a + b - c
            for u, v, k in path:
                del at_s[u, k], at_d[v, k]
            for u, v, k in path:
                at_s[u, a + b - k], at_d[v, a + b - k] = v, u
        at_s[s, a], at_d[d, a] = d, s
    return [sorted((s, d) for (s, k), d in at_s.items() if k == c) for c in range(count)]


def make_plan():
    low, high = row_bounds()
    items = wanted(low, high)
    by_class = [[] for _ in CLASSES]
    for code in ROUTES:
        blocks, kind, d, s = code % 32, code // 32 % 16, code // 512 % 64, code // 32768
        by_class[kind] += [(s, d)] * blocks
    slots, left = [], {e: list(v) for e, v in items.items()}
    for (kind, size, count), edges in zip(CLASSES, by_class):
        for pairs in colour(edges, count):
            slots.append((kind, size, pairs))
    slots = [slots[j] for j in SLOTS]
    total = sum(size for _, size, _ in slots)
    send = np.zeros((ROWS, 1, total), np.int32)
    sends = np.zeros((ROWS, len(slots)), np.int32)
    near = np.full(ROWS, ROWS - SPAN)
    merc = np.full((ROWS, OWN), -1, np.int32)
    base = np.array([low[OWN * d] for d in range(ROWS)])
    width = max(high[OWN * d + OWN - 1] + 2 - base[d] for d in range(ROWS))
    place = np.zeros((ROWS, width), np.int32)
    used = np.zeros((ROWS, len(slots)), np.int32)
    at = 0
    for j, (kind, size, pairs) in enumerate(slots):
        for s, d in pairs:
            block, left[s, d] = left[s, d][:size], left[s, d][size:]
            used[d, j] = sends[s, j] = 1 if block else 0
            for k, (what, r) in enumerate(block):
                if what == "m":
                    send[s, 0, at + k] = CODE + r
                    near[s] = min(near[s], d)
                    merc[d, r - OWN * d] = at + k
                else:
                    send[s, 0, at + k] = r - OWN * s
                    place[d, r - base[d]] = at + k
        at += size
    assert not any(left.values())
    take = np.concatenate([used, base[:, None].astype(np.int32), merc, place], axis=1)[:, None, :]
    for s in range(ROWS):
        codes = send[s, 0]
        codes[codes >= CODE] -= OWN * near[s]
        assert codes.max() < CODE + SPAN * OWN
    send = np.concatenate([near[:, None, None], sends[:, None, :], send], axis=2)
    return slots, send.astype(np.int32), take.astype(np.int32)


def hops(slot):
    kind, _, pairs = slot
    tracks = []
    for s, d in pairs:
        track = [s]
        for dz, dx in STOPS[kind]:
            track.append(stop(track[-1], dz, dx))
        tracks.append(track + [d])
    return [[(t[i], t[i + 1]) for t in tracks] for i in range(len(tracks[0]) - 1)]


def pack_rows(slots, group, source, send, me, low_row, weight_low):
    starts = np.cumsum([1 + len(slots)] + [size for _, size, _ in slots])
    sizes = [slots[j][1] for j in group]

    def kernel(me_ref, send_ref, low_ref, weight_ref, source_ref, *refs):
        outs, (lows, weights, sems) = refs[: len(group)], refs[len(group) :]
        begin = me_ref[0] * OWN
        near = send_ref[0, 0, 0]
        copies = [
            pltpu.make_async_copy(low_ref.at[pl.ds(near, SPAN)], lows, sems.at[0]),
            pltpu.make_async_copy(weight_ref.at[pl.ds(near, SPAN)], weights, sems.at[1]),
        ]
        for copy in copies:
            copy.start()
        for copy in copies:
            copy.wait()
        for j, out, size in zip(group, outs, sizes):

            def row(k, _, out=out, at=int(starts[j])):
                code = send_ref[0, 0, at + k]
                mixed = code >= CODE
                m = jnp.maximum(code - CODE, 0)
                a, b = lax.shift_right_logical(m, 7), lax.bitwise_and(m, OWN - 1)
                r0 = jnp.where(mixed, jnp.clip(lows[a, 0, b] - begin, 0, OWN - 2), code)
                r1 = jnp.where(mixed, r0 + 1, r0)
                w = jnp.where(mixed, weights[a, 0, b], 1.0)
                v = 1.0 - w
                b0 = lax.shift_right_logical(r0, 3) * 512 + lax.bitwise_and(r0, 7)
                b1 = lax.shift_right_logical(r1, 3) * 512 + lax.bitwise_and(r1, 7)
                for c in range(8):
                    x = source_ref[pl.ds(b0 + 64 * c, 8, stride=8), :]
                    y = source_ref[pl.ds(b1 + 64 * c, 8, stride=8), :]
                    out[pl.ds(pl.multiple_of(k * 64 + 8 * c, 8), 8), :] = w * x + v * y
                return 0

            @pl.when(send_ref[0, 0, 1 + j] > 0)
            def _(row=row, size=size):
                lax.fori_loop(0, size, row, 0, unroll=8)

    total = send.shape[-1]
    return pl.pallas_call(
        kernel,
        grid_spec=pltpu.PrefetchScalarGridSpec(
            num_scalar_prefetch=1,
            grid=(1,),
            in_specs=[
                pl.BlockSpec((1, 1, total), lambda i, q: (q[0], 0, 0), memory_space=pltpu.SMEM),
                pl.BlockSpec(memory_space=pl.ANY),
                pl.BlockSpec(memory_space=pl.ANY),
                pl.BlockSpec(memory_space=pltpu.VMEM),
            ],
            out_specs=[pl.BlockSpec(memory_space=pltpu.VMEM) for _ in sizes],
            scratch_shapes=[
                pltpu.SMEM((SPAN, 1, OWN), jnp.int32),
                pltpu.SMEM((SPAN, 1, OWN), jnp.float32),
                pltpu.SemaphoreType.DMA((2,)),
            ],
        ),
        out_shape=[pltpu.VMEM((size * 64, 128), jnp.float32) for size in sizes],
        compiler_params=pltpu.CompilerParams(vmem_limit_bytes=8 << 20),
        name="pack_rows",
    )(me, send, low_row, weight_low, source)


def finish(slots, blocks, take, me, low_row, weight_low):
    sizes = [size for _, size, _ in slots]
    starts = np.cumsum([0] + sizes)
    n = len(slots)
    width = take.shape[-1] - n - 1 - OWN

    def pooled(sums, first, rows):
        pair = jnp.concatenate(
            [sums[pl.ds(first, rows // 2, stride=2), :], sums[pl.ds(first + 1, rows // 2, stride=2), :]], axis=1
        )
        lane = lax.broadcasted_iota(jnp.int32, (256, 128), 0)
        to = lax.broadcasted_iota(jnp.int32, (256, 128), 1)
        pairing = jnp.where(lax.div(lane, 2) == to, 0.25, 0.0).astype(jnp.bfloat16)
        high = pair.astype(jnp.bfloat16)
        low = (pair - high.astype(jnp.float32)).astype(jnp.bfloat16)
        return sum(jnp.dot(part, pairing, preferred_element_type=jnp.float32) for part in (low, high))

    def kernel(me_ref, take_ref, low_ref, weight_ref, *refs):
        ins, (out, out1, out2, *smalls), (got, sums, ones, sems) = refs[:n], refs[n : n + 7], refs[n + 7 :]
        step = pl.program_id(0)

        @pl.when(step == 0)
        def _():
            def copy(j):
                return pltpu.make_async_copy(ins[j], got.at[pl.ds(int(starts[j]) * 64, sizes[j] * 64), :], sems.at[j])

            for j in range(n):

                @pl.when(take_ref[0, 0, j] > 0)
                def _(j=j):
                    copy(j).start()

            for j in range(n):

                @pl.when(take_ref[0, 0, j] > 0)
                def _(j=j):
                    copy(j).wait()

        base = take_ref[0, 0, n]

        def blended(r):
            i = step * 32 + r
            fixed = take_ref[0, 0, n + 1 + i]
            c = jnp.clip(low_ref[0, 0, i] - base, 0, width - 2)
            p0 = take_ref[0, 0, n + 1 + OWN + c]
            p1 = take_ref[0, 0, n + 2 + OWN + c]
            done = fixed >= 0
            p0 = jnp.where(done, fixed, p0)
            p1 = jnp.where(done, fixed, p1)
            w = jnp.where(done, 1.0, weight_ref[0, 0, i])
            v = 1.0 - w
            for j in range(8):
                a = got[pl.ds(pl.multiple_of(p0 * 64 + 8 * j, 8), 8), :]
                b = got[pl.ds(pl.multiple_of(p1 * 64 + 8 * j, 8), 8), :]
                yield j, w * a + v * b

        for r in range(0, 32, 2):
            for (j, a), (_, b) in zip(blended(r), blended(r + 1)):
                out[pl.ds(r // 8 * 512 + r % 8 + 64 * j, 8, stride=8), :] = a
                out[pl.ds(r // 8 * 512 + r % 8 + 1 + 64 * j, 8, stride=8), :] = b
                sums[pl.ds(r * 32 + 8 * j, 8), :] = a + b
        for half in range(2):
            one = pooled(sums, half * 512, 512)
            for r in range(8):
                for j in range(4):
                    out1[pl.ds(half * 256 + r + 64 * j, 8, stride=8), :] = one[r * 32 + 8 * j : r * 32 + 8 * j + 8]
            for r in range(4):
                ones[pl.ds(step * 256 + half * 128 + r * 32, 32), :] = (
                    one[r * 64 : r * 64 + 32] + one[r * 64 + 32 : r * 64 + 64]
                )

        @pl.when(step == 3)
        def _():
            two = pooled(ones, 0, 1024)
            for r in range(32):
                for j in range(2):
                    out2[pl.ds(r // 8 * 128 + r % 8 + 64 * j, 8, stride=8), :] = two[r * 16 + 8 * j : r * 16 + 8 * j + 8]
            for r in range(16):
                sums[pl.ds(r * 16, 16), :] = two[r * 32 : r * 32 + 16] + two[r * 32 + 16 : r * 32 + 32]
            three = pooled(sums, 0, 256)
            ones[pl.ds(0, 128), :] = three
            for r in range(8):
                sums[pl.ds(r * 8, 8), :] = three[r * 16 : r * 16 + 8] + three[r * 16 + 8 : r * 16 + 16]
            ones[pl.ds(128, 32), :] = pooled(sums, 0, 64)
            for k, small in enumerate(smalls):
                c = lax.rem(me_ref[1] + k, 4)
                small[pl.ds(0, 32), :] = ones[pl.ds(pl.multiple_of(c * 32, 8), 32), :]
                small[pl.ds(32, 8), :] = ones[pl.ds(pl.multiple_of(128 + c * 8, 8), 8), :]

    return pl.pallas_call(
        kernel,
        grid_spec=pltpu.PrefetchScalarGridSpec(
            num_scalar_prefetch=1,
            grid=(4,),
            in_specs=[
                pl.BlockSpec((1, 1, take.shape[-1]), lambda i, q: (q[0], 0, 0), memory_space=pltpu.SMEM),
                pl.BlockSpec((1, 1, OWN), lambda i, q: (q[0], 0, 0), memory_space=pltpu.SMEM),
                pl.BlockSpec((1, 1, OWN), lambda i, q: (q[0], 0, 0), memory_space=pltpu.SMEM),
            ]
            + [pl.BlockSpec(memory_space=pl.ANY)] * n,
            out_specs=[
                pl.BlockSpec((2048, 128), lambda i, q: (i, 0)),
                pl.BlockSpec((512, 128), lambda i, q: (i, 0)),
                pl.BlockSpec((512, 128), lambda i, q: (0, 0)),
            ]
            + [pl.BlockSpec((40, 128), lambda i, q: (0, 0))] * 4,
            scratch_shapes=[
                pltpu.VMEM((int(starts[-1]) * 64, 128), jnp.float32),
                pltpu.VMEM((1024, 128), jnp.float32),
                pltpu.VMEM((1024, 128), jnp.float32),
                pltpu.SemaphoreType.DMA((n,)),
            ],
        ),
        out_shape=[
            jax.ShapeDtypeStruct((8192, 128), jnp.float32),
            jax.ShapeDtypeStruct((2048, 128), jnp.float32),
            jax.ShapeDtypeStruct((512, 128), jnp.float32),
        ]
        + [jax.ShapeDtypeStruct((40, 128), jnp.float32)] * 4,
        compiler_params=pltpu.CompilerParams(dimension_semantics=("arbitrary",), vmem_limit_bytes=20 << 20),
        name="finish",
    )(me, take, low_row, weight_low, *blocks)


def join(pieces, me):
    def kernel(me_ref, *refs):
        ins, (three, four) = refs[:4], refs[4:]
        for k, piece in enumerate(ins):
            c = lax.rem(me_ref[1] + 4 - k, 4)
            for t in range(8):
                three[:, pl.ds(pl.multiple_of(c * 1024 + 128 * t, 128), 128)] = piece[pl.ds(t, 4, stride=8), :]
            for t in range(4):
                four[:, pl.ds(pl.multiple_of(c * 512 + 128 * t, 128), 128)] = piece[pl.ds(32 + t, 2, stride=4), :]

    return pl.pallas_call(
        kernel,
        in_specs=[pl.BlockSpec(memory_space=pltpu.SMEM)] + [pl.BlockSpec(memory_space=pltpu.VMEM)] * 4,
        out_shape=[jax.ShapeDtypeStruct((4, 4096), jnp.float32), jax.ShapeDtypeStruct((2, 2048), jnp.float32)],
        compiler_params=pltpu.CompilerParams(vmem_limit_bytes=4 << 20),
        name="join",
    )(me, *pieces)


def tiled(flat, rows, cols):
    return flat.reshape(rows // 8, cols // 128, 8, 128).transpose(0, 2, 1, 3).reshape(rows, cols)


def solution(mesh):
    slots, send, take = make_plan()
    groups = [range(3), range(3, len(slots))]
    order = [divmod(code, 2) for code in ISSUE]

    def body(source, low_row, weight_low):
        me = jnp.stack([lax.axis_index("rows"), lax.axis_index("cols")]).astype(jnp.int32)
        flat = source.reshape(16, 8, 64, 128).transpose(0, 2, 1, 3).reshape(TOTAL, 128)
        flat = pltpu.with_memory_space_constraint(flat, pltpu.VMEM)
        low_row = low_row.reshape(ROWS, 1, OWN)
        weight_low = weight_low.reshape(ROWS, 1, OWN)
        low_row = pltpu.with_memory_space_constraint(low_row, pltpu.HBM)
        weight_low = pltpu.with_memory_space_constraint(weight_low, pltpu.HBM)
        sends = pltpu.with_memory_space_constraint(jnp.asarray(send), pltpu.HBM)
        takes = pltpu.with_memory_space_constraint(jnp.asarray(take), pltpu.HBM)
        packed = []
        for group in groups:
            packed += pack_rows(slots, group, flat, sends, me, low_row, weight_low)
        blocks = [[b] for b in packed]
        tracks = [hops(slot) for slot in slots]
        for j, i in order:
            blocks[j].append(lax.ppermute(blocks[j][-1], "rows", tracks[j][i]))
        out, out1, out2, *smalls = finish(slots, [b[-1] for b in blocks], takes, me, low_row, weight_low)
        pieces = smalls[:1]
        for k in (2, 1, 3):
            pieces.append(lax.ppermute(smalls[k], "cols", [(c, (c + k) % 4) for c in range(4)]))
        level3, level4 = join([pieces[0], pieces[2], pieces[1], pieces[3]], me)
        return (
            tiled(out, 128, 8192),
            tiled(out1, 64, 4096),
            tiled(out2, 32, 2048),
            level3,
            level4,
        )

    return jax.shard_map(
        body,
        mesh=mesh,
        in_specs=(P("rows", "cols"), P(), P()),
        out_specs=(
            P("rows", "cols"),
            P("rows", "cols"),
            P("rows", "cols"),
            P(("rows", "cols"), None),
            P(("rows", "cols"), None),
        ),
        check_vma=False,
    )
```

```python
import math

import jax
import jax.numpy as jnp
import numpy as np
from jax import lax
from jax.experimental import pallas as pl
from jax.experimental.pallas import tpu as pltpu
from jax.sharding import PartitionSpec as P


TOTAL = 8192
ROWS = 64
OWN = TOTAL // ROWS
SLOTS = (13, 6, 9, 3, 12, 11, 7, 10, 4, 0, 1, 2, 14, 5, 8)
ISSUE = (0, 2, 4, 6, 8, 10, 12, 14, 16, 18, 20, 22, 24, 11, 5, 9, 1, 26, 25, 15, 28)
SPAN = 3
CODE = 1024

STOPS = {
    "D": (),
    "P": ((0, 1),),
    "M": ((0, -1),),
    "N": ((-4, 0),),
    "O": ((-3, 0),),
    "V": ((1, -1),),
    "Y": ((-1, -1),),
}
CLASSES = (("D", 32, 3), ("D", 16, 3), ("D", 8, 3), ("P", 32, 1), ("M", 32, 1), ("Y", 16, 1), ("V", 16, 1), ("N", 24, 1), ("O", 24, 1))
ROUTES = (
    1632961, 503297, 1068547, 836321, 736259, 1268225, 1135139, 1500161, 1466977, 1400866, 1532993, 1964034,
    1997314, 1069090, 369313, 1964610, 536577, 1533025, 536066, 1732098, 1997377, 2063394, 369377, 336385,
    1101889, 969249, 1599523, 1533506, 1599681, 134689, 1135169, 335425, 1334433, 302594, 969281, 1035841,
    469601, 1665570, 1665601, 702497, 968770, 1267714, 502785, 1666209, 269346, 436449, 1002018, 67137,
    1566273, 2030081, 1234945, 569922, 302145, 502817, 135202, 33825, 201761, 1500289, 669249, 1798145,
    603201, 1698850, 1764929, 836098, 1400385, 202241, 1267745, 168994, 1002497, 1964065, 802850, 1798209,
    1001985, 1732161, 1234498, 1931297, 1035809, 503329, 1434177, 868897, 868929, 2063939, 236097, 602625,
    1599553, 1831426, 403073, 836129, 1466913, 1201153, 469537, 669729, 436226, 469505, 669698, 1101857,
    1367074, 1300994, 469571, 269313, 669953, 1135233, 545, 1698881, 67105, 502881, 968738, 1897505,
    68097, 436257, 1897986, 1102402, 669217, 1135105, 135169, 168577, 435777, 369730, 1400897, 1168033,
    569409, 703042, 303169, 1002561, 336001, 1599489, 1765378, 1566721, 335907, 67586, 1035330, 34305,
    168481, 578, 869441, 235041, 536833, 1798657, 1566785, 1699489, 68161, 101441, 2, 1930753,
    1201217, 101921, 236065, 603138, 1666049, 1168449, 536129, 902881, 869409, 402978, 435745, 1898017,
    935489, 1367745, 1168418, 570113, 1632833, 1234465, 636418, 769538, 702978, 1831970, 235522, 736513,
    101378, 902658, 802337, 201793, 869378, 1333825, 1931265, 101409, 902145, 1765569, 369697, 168513,
    1931329, 769793, 569857, 736321, 513, 100897, 302626, 1732130, 1400353, 1301121, 2030625, 201889,
    335937, 935425, 1433601, 1400993, 1864769, 1235201, 34369, 1798753, 1466882, 636482, 2096643, 1201697,
    436769, 536609, 836161, 803041, 369153, 1930785, 34337, 202274, 503361, 769090, 1301025, 703009,
    669761, 403009, 302081, 235073, 336033, 268866, 167937, 569889, 636673, 33794, 869601, 1533475,
    769633, 403169, 1434273, 635905, 168449, 1334275, 603393, 1500194, 1002721, 569377, 1666113, 1632770,
    1997346, 936161, 1632321, 1765537, 902721, 1035266, 100865, 2030594, 1699393, 602689, 33313, 502849,
    1102081, 1433665, 268802, 1499681, 1964097, 1433633, 235617, 769601, 1566210, 1898049, 470017, 336449,
    1666241, 1234561, 1831457, 569345, 1301569, 1699521, 2063905, 402465, 1267777, 2063361, 65, 802818,
    703233, 1367554, 1864707, 935938, 735777, 1930817, 835617, 969217, 67617, 1168386, 436289, 1201666,
    1433729, 402433, 969441, 1400417, 1632801, 1698817, 201825, 1101826, 369793, 1036001, 134658, 202305,
)


def row_bounds():
    top = 68.0 * math.pi / 180.0
    edge = math.log(math.tan(math.pi / 4 + top / 2))
    y = edge * (1 - (2 * np.arange(TOTAL) + 1) / (2.0 * TOTAL))
    position = (top - (2 * np.arctan(np.exp(y)) - math.pi / 2)) / top * TOTAL - 0.5
    low = np.clip(np.floor(position - 0.05), 0, TOTAL - 2) - 2
    high = np.clip(np.floor(position + 0.05), 0, TOTAL - 2) + 2
    return np.clip(low, 0, TOTAL - 2).astype(int), np.clip(high, 0, TOTAL - 2).astype(int)


def wanted(low, high):
    out = {}
    for d in range(ROWS):
        mine = range(OWN * d, OWN * d + OWN)
        first, last = low[mine[0]], high[mine[-1]] + 1
        for s in range(first // OWN, last // OWN + 1):
            begin, end = s * OWN, s * OWN + OWN - 1
            plain = [("s", r) for r in range(max(first, begin), min(last, end) + 1)]
            inside = [m for m in mine if low[m] >= begin and high[m] + 1 <= end]
            across = sorted({
                r for m in mine if m not in inside for r in range(low[m], high[m] + 2) if r // OWN == s
            })
            mixed = [("s", r) for r in across if r < begin + OWN // 2]
            mixed += [("m", m) for m in inside]
            mixed += [("s", r) for r in across if r >= begin + OWN // 2]
            out[s, d] = plain if len(plain) <= len(mixed) else mixed
    return out


def stop(q, dz, dx):
    z, x = q // 8, q % 8 // 2
    return (z + dz) % 8 * 8 + (x + dx) % 4 * 2 + q % 2


def colour(edges, count):
    at_s, at_d = {}, {}
    for s, d in edges:
        a = next(c for c in range(count) if (s, c) not in at_s)
        b = next(c for c in range(count) if (d, c) not in at_d)
        if a != b:
            path, node, side, c = [], d, 1, a
            while True:
                table = at_d if side else at_s
                if (node, c) not in table:
                    break
                other = table[node, c]
                path.append((other, node, c) if side else (node, other, c))
                node, side, c = other, 1 - side, a + b - c
            for u, v, k in path:
                del at_s[u, k], at_d[v, k]
            for u, v, k in path:
                at_s[u, a + b - k], at_d[v, a + b - k] = v, u
        at_s[s, a], at_d[d, a] = d, s
    return [sorted((s, d) for (s, k), d in at_s.items() if k == c) for c in range(count)]


def make_plan():
    low, high = row_bounds()
    items = wanted(low, high)
    by_class = [[] for _ in CLASSES]
    for code in ROUTES:
        blocks, kind, d, s = code % 32, code // 32 % 16, code // 512 % 64, code // 32768
        by_class[kind] += [(s, d)] * blocks
    slots, left = [], {e: list(v) for e, v in items.items()}
    for (kind, size, count), edges in zip(CLASSES, by_class):
        for pairs in colour(edges, count):
            slots.append((kind, size, pairs))
    slots = [slots[j] for j in SLOTS]
    total = sum(size for _, size, _ in slots)
    send = np.zeros((ROWS, 1, total), np.int32)
    sends = np.zeros((ROWS, len(slots)), np.int32)
    near = np.full(ROWS, ROWS - SPAN)
    merc = np.full((ROWS, OWN), -1, np.int32)
    base = np.array([low[OWN * d] for d in range(ROWS)])
    width = max(high[OWN * d + OWN - 1] + 2 - base[d] for d in range(ROWS))
    place = np.zeros((ROWS, width), np.int32)
    used = np.zeros((ROWS, len(slots)), np.int32)
    at = 0
    for j, (kind, size, pairs) in enumerate(slots):
        for s, d in pairs:
            block, left[s, d] = left[s, d][:size], left[s, d][size:]
            used[d, j] = sends[s, j] = 1 if block else 0
            for k, (what, r) in enumerate(block):
                if what == "m":
                    send[s, 0, at + k] = CODE + r
                    near[s] = min(near[s], d)
                    merc[d, r - OWN * d] = at + k
                else:
                    send[s, 0, at + k] = r - OWN * s
                    place[d, r - base[d]] = at + k
        at += size
    assert not any(left.values())
    take = np.concatenate([used, base[:, None].astype(np.int32), merc, place], axis=1)[:, None, :]
    for s in range(ROWS):
        codes = send[s, 0]
        codes[codes >= CODE] -= OWN * near[s]
        assert codes.max() < CODE + SPAN * OWN
    send = np.concatenate([near[:, None, None], sends[:, None, :], send], axis=2)
    return slots, send.astype(np.int32), take.astype(np.int32)


def hops(slot):
    kind, _, pairs = slot
    tracks = []
    for s, d in pairs:
        track = [s]
        for dz, dx in STOPS[kind]:
            track.append(stop(track[-1], dz, dx))
        tracks.append(track + [d])
    return [[(t[i], t[i + 1]) for t in tracks] for i in range(len(tracks[0]) - 1)]


def pack_rows(slots, group, source, send, me, low_row, weight_low):
    starts = np.cumsum([1 + len(slots)] + [size for _, size, _ in slots])
    sizes = [slots[j][1] for j in group]

    def kernel(me_ref, send_ref, low_ref, weight_ref, source_ref, *refs):
        outs, (lows, weights, sems) = refs[: len(group)], refs[len(group) :]
        begin = me_ref[0] * OWN
        near = send_ref[0, 0, 0]
        copies = [
            pltpu.make_async_copy(low_ref.at[pl.ds(near, SPAN)], lows, sems.at[0]),
            pltpu.make_async_copy(weight_ref.at[pl.ds(near, SPAN)], weights, sems.at[1]),
        ]
        for copy in copies:
            copy.start()
        for copy in copies:
            copy.wait()
        for j, out, size in zip(group, outs, sizes):

            def row(k, _, out=out, at=int(starts[j])):
                code = send_ref[0, 0, at + k]
                mixed = code >= CODE
                m = jnp.maximum(code - CODE, 0)
                a, b = lax.shift_right_logical(m, 7), lax.bitwise_and(m, OWN - 1)
                r0 = jnp.where(mixed, jnp.clip(lows[a, 0, b] - begin, 0, OWN - 2), code)
                r1 = jnp.where(mixed, r0 + 1, r0)
                w = jnp.where(mixed, weights[a, 0, b], 1.0)
                v = 1.0 - w
                b0 = lax.shift_right_logical(r0, 3) * 512 + lax.bitwise_and(r0, 7)
                b1 = lax.shift_right_logical(r1, 3) * 512 + lax.bitwise_and(r1, 7)
                for c in range(8):
                    x = source_ref[pl.ds(b0 + 64 * c, 8, stride=8), :]
                    y = source_ref[pl.ds(b1 + 64 * c, 8, stride=8), :]
                    out[pl.ds(pl.multiple_of(k * 64 + 8 * c, 8), 8), :] = w * x + v * y
                return 0

            @pl.when(send_ref[0, 0, 1 + j] > 0)
            def _(row=row, size=size):
                lax.fori_loop(0, size, row, 0, unroll=8)

    total = send.shape[-1]
    return pl.pallas_call(
        kernel,
        grid_spec=pltpu.PrefetchScalarGridSpec(
            num_scalar_prefetch=1,
            grid=(1,),
            in_specs=[
                pl.BlockSpec((1, 1, total), lambda i, q: (q[0], 0, 0), memory_space=pltpu.SMEM),
                pl.BlockSpec(memory_space=pl.ANY),
                pl.BlockSpec(memory_space=pl.ANY),
                pl.BlockSpec(memory_space=pltpu.VMEM),
            ],
            out_specs=[pl.BlockSpec(memory_space=pltpu.VMEM) for _ in sizes],
            scratch_shapes=[
                pltpu.SMEM((SPAN, 1, OWN), jnp.int32),
                pltpu.SMEM((SPAN, 1, OWN), jnp.float32),
                pltpu.SemaphoreType.DMA((2,)),
            ],
        ),
        out_shape=[pltpu.VMEM((size * 64, 128), jnp.float32) for size in sizes],
        compiler_params=pltpu.CompilerParams(vmem_limit_bytes=8 << 20),
        name="pack_rows",
    )(me, send, low_row, weight_low, source)


def finish(slots, blocks, take, me, low_row, weight_low):
    sizes = [size for _, size, _ in slots]
    starts = np.cumsum([0] + sizes)
    n = len(slots)
    width = take.shape[-1] - n - 1 - OWN

    def pooled(sums, first, rows):
        pair = jnp.concatenate(
            [sums[pl.ds(first, rows // 2, stride=2), :], sums[pl.ds(first + 1, rows // 2, stride=2), :]], axis=1
        )
        lane = lax.broadcasted_iota(jnp.int32, (256, 128), 0)
        to = lax.broadcasted_iota(jnp.int32, (256, 128), 1)
        pairing = jnp.where(lax.div(lane, 2) == to, 0.25, 0.0).astype(jnp.bfloat16)
        high = pair.astype(jnp.bfloat16)
        low = (pair - high.astype(jnp.float32)).astype(jnp.bfloat16)
        return sum(jnp.dot(part, pairing, preferred_element_type=jnp.float32) for part in (low, high))

    def kernel(me_ref, take_ref, low_ref, weight_ref, *refs):
        ins, (out, out1, out2, *smalls), (got, sums, ones, sems) = refs[:n], refs[n : n + 7], refs[n + 7 :]
        step = pl.program_id(0)

        @pl.when(step == 0)
        def _():
            def copy(j):
                return pltpu.make_async_copy(ins[j], got.at[pl.ds(int(starts[j]) * 64, sizes[j] * 64), :], sems.at[j])

            for j in range(n):

                @pl.when(take_ref[0, 0, j] > 0)
                def _(j=j):
                    copy(j).start()

            for j in range(n):

                @pl.when(take_ref[0, 0, j] > 0)
                def _(j=j):
                    copy(j).wait()

        base = take_ref[0, 0, n]

        def blended(r):
            i = step * 32 + r
            fixed = take_ref[0, 0, n + 1 + i]
            c = jnp.clip(low_ref[0, 0, i] - base, 0, width - 2)
            p0 = take_ref[0, 0, n + 1 + OWN + c]
            p1 = take_ref[0, 0, n + 2 + OWN + c]
            done = fixed >= 0
            p0 = jnp.where(done, fixed, p0)
            p1 = jnp.where(done, fixed, p1)
            w = jnp.where(done, 1.0, weight_ref[0, 0, i])
            v = 1.0 - w
            for j in range(8):
                a = got[pl.ds(pl.multiple_of(p0 * 64 + 8 * j, 8), 8), :]
                b = got[pl.ds(pl.multiple_of(p1 * 64 + 8 * j, 8), 8), :]
                yield j, w * a + v * b

        for r in range(0, 32, 2):
            for (j, a), (_, b) in zip(blended(r), blended(r + 1)):
                out[pl.ds(r // 8 * 512 + r % 8 + 64 * j, 8, stride=8), :] = a
                out[pl.ds(r // 8 * 512 + r % 8 + 1 + 64 * j, 8, stride=8), :] = b
                sums[pl.ds(r * 32 + 8 * j, 8), :] = a + b
        for half in range(2):
            one = pooled(sums, half * 512, 512)
            for r in range(8):
                for j in range(4):
                    out1[pl.ds(half * 256 + r + 64 * j, 8, stride=8), :] = one[r * 32 + 8 * j : r * 32 + 8 * j + 8]
            for r in range(4):
                ones[pl.ds(step * 256 + half * 128 + r * 32, 32), :] = (
                    one[r * 64 : r * 64 + 32] + one[r * 64 + 32 : r * 64 + 64]
                )

        @pl.when(step == 3)
        def _():
            two = pooled(ones, 0, 1024)
            for r in range(32):
                for j in range(2):
                    out2[pl.ds(r // 8 * 128 + r % 8 + 64 * j, 8, stride=8), :] = two[r * 16 + 8 * j : r * 16 + 8 * j + 8]
            for r in range(16):
                sums[pl.ds(r * 16, 16), :] = two[r * 32 : r * 32 + 16] + two[r * 32 + 16 : r * 32 + 32]
            three = pooled(sums, 0, 256)
            ones[pl.ds(0, 128), :] = three
            for r in range(8):
                sums[pl.ds(r * 8, 8), :] = three[r * 16 : r * 16 + 8] + three[r * 16 + 8 : r * 16 + 16]
            ones[pl.ds(128, 32), :] = pooled(sums, 0, 64)
            for k, small in enumerate(smalls):
                c = lax.rem(me_ref[1] + k, 4)
                small[pl.ds(0, 32), :] = ones[pl.ds(pl.multiple_of(c * 32, 8), 32), :]
                small[pl.ds(32, 8), :] = ones[pl.ds(pl.multiple_of(128 + c * 8, 8), 8), :]

    return pl.pallas_call(
        kernel,
        grid_spec=pltpu.PrefetchScalarGridSpec(
            num_scalar_prefetch=1,
            grid=(4,),
            in_specs=[
                pl.BlockSpec((1, 1, take.shape[-1]), lambda i, q: (q[0], 0, 0), memory_space=pltpu.SMEM),
                pl.BlockSpec((1, 1, OWN), lambda i, q: (q[0], 0, 0), memory_space=pltpu.SMEM),
                pl.BlockSpec((1, 1, OWN), lambda i, q: (q[0], 0, 0), memory_space=pltpu.SMEM),
            ]
            + [pl.BlockSpec(memory_space=pl.ANY)] * n,
            out_specs=[
                pl.BlockSpec((2048, 128), lambda i, q: (i, 0)),
                pl.BlockSpec((512, 128), lambda i, q: (i, 0)),
                pl.BlockSpec((512, 128), lambda i, q: (0, 0)),
            ]
            + [pl.BlockSpec((40, 128), lambda i, q: (0, 0))] * 4,
            scratch_shapes=[
                pltpu.VMEM((int(starts[-1]) * 64, 128), jnp.float32),
                pltpu.VMEM((1024, 128), jnp.float32),
                pltpu.VMEM((1024, 128), jnp.float32),
                pltpu.SemaphoreType.DMA((n,)),
            ],
        ),
        out_shape=[
            jax.ShapeDtypeStruct((8192, 128), jnp.float32),
            jax.ShapeDtypeStruct((2048, 128), jnp.float32),
            jax.ShapeDtypeStruct((512, 128), jnp.float32),
        ]
        + [jax.ShapeDtypeStruct((40, 128), jnp.float32)] * 4,
        compiler_params=pltpu.CompilerParams(dimension_semantics=("arbitrary",), vmem_limit_bytes=20 << 20),
        name="finish",
    )(me, take, low_row, weight_low, *blocks)


def join(pieces, me):
    def kernel(me_ref, *refs):
        ins, (three, four) = refs[:4], refs[4:]
        for k, piece in enumerate(ins):
            c = lax.rem(me_ref[1] + 4 - k, 4)
            for t in range(8):
                three[:, pl.ds(pl.multiple_of(c * 1024 + 128 * t, 128), 128)] = piece[pl.ds(t, 4, stride=8), :]
            for t in range(4):
                four[:, pl.ds(pl.multiple_of(c * 512 + 128 * t, 128), 128)] = piece[pl.ds(32 + t, 2, stride=4), :]

    return pl.pallas_call(
        kernel,
        in_specs=[pl.BlockSpec(memory_space=pltpu.SMEM)] + [pl.BlockSpec(memory_space=pltpu.VMEM)] * 4,
        out_shape=[jax.ShapeDtypeStruct((4, 4096), jnp.float32), jax.ShapeDtypeStruct((2, 2048), jnp.float32)],
        compiler_params=pltpu.CompilerParams(vmem_limit_bytes=4 << 20),
        name="join",
    )(me, *pieces)


def tiled(flat, rows, cols):
    return flat.reshape(rows // 8, cols // 128, 8, 128).transpose(0, 2, 1, 3).reshape(rows, cols)


def solution(mesh):
    slots, send, take = make_plan()
    groups = [range(3), range(3, len(slots))]
    order = [divmod(code, 2) for code in ISSUE]

    def body(source, low_row, weight_low):
        me = jnp.stack([lax.axis_index("rows"), lax.axis_index("cols")]).astype(jnp.int32)
        flat = source.reshape(16, 8, 64, 128).transpose(0, 2, 1, 3).reshape(TOTAL, 128)
        flat = pltpu.with_memory_space_constraint(flat, pltpu.VMEM)
        low_row = low_row.reshape(ROWS, 1, OWN)
        weight_low = weight_low.reshape(ROWS, 1, OWN)
        low_row = pltpu.with_memory_space_constraint(low_row, pltpu.HBM)
        weight_low = pltpu.with_memory_space_constraint(weight_low, pltpu.HBM)
        sends = pltpu.with_memory_space_constraint(jnp.asarray(send), pltpu.HBM)
        takes = pltpu.with_memory_space_constraint(jnp.asarray(take), pltpu.HBM)
        packed = []
        for group in groups:
            packed += pack_rows(slots, group, flat, sends, me, low_row, weight_low)
        blocks = [[b] for b in packed]
        tracks = [hops(slot) for slot in slots]
        for j, i in order:
            blocks[j].append(lax.ppermute(blocks[j][-1], "rows", tracks[j][i]))
        out, out1, out2, *smalls = finish(slots, [b[-1] for b in blocks], takes, me, low_row, weight_low)
        pieces = smalls[:1]
        for k in (2, 1, 3):
            pieces.append(lax.ppermute(smalls[k], "cols", [(c, (c + k) % 4) for c in range(4)]))
        level3, level4 = join([pieces[0], pieces[2], pieces[1], pieces[3]], me)
        return (
            tiled(out, 128, 8192),
            tiled(out1, 64, 4096),
            tiled(out2, 32, 2048),
            level3,
            level4,
        )

    return jax.shard_map(
        body,
        mesh=mesh,
        in_specs=(P("rows", "cols"), P(), P()),
        out_specs=(
            P("rows", "cols"),
            P("rows", "cols"),
            P("rows", "cols"),
            P(("rows", "cols"), None),
            P(("rows", "cols"), None),
        ),
        check_vma=False,
    )
```
